256 devices in a mesh: atoms: 128 (over x, z, y), vecs: 2 (over core).
Axes of the slice: x: 4, y: 4, z: 8, core: 2. Of those that a mesh axis runs over, the one named last changes fastest.
Arguments:
- start_block: bfloat16 [65536, 1024], P('atoms', 'vecs'), may hold values from -6 to 6
- onsite: bfloat16 [512, 128, 128], P('atoms'), may hold values from -0.15625 to 0.15625
- hopping: bfloat16 [512, 4, 128, 128], P('atoms'), as said below
- columns: int32 [512, 4], P('atoms'), may hold values from 0 to 511, as said below
- counts: int32 [512], P('atoms'), may hold values from 0 to 4, as said below
Outputs:
- filtered: bfloat16 [65536, 1024], P('atoms', 'vecs')
- gram: float32 [1024, 1024], P('atoms', 'vecs')
- projected: float32 [1024, 1024], P('atoms', 'vecs')
The draws below stay inside these ranges and needn't reach their ends.
Inputs may be any that keep to these rules, and one draw needn't show every extreme that they name: `columns`: each block row lists its live neighbours in its first counts[i] slots; every neighbour lies at most 2 blocks away, counted cyclically over the 512 blocks; the neighbour relation is symmetric; the other slots name blocks within the same reach that are not neighbours. `counts`: some block row has all 4 slots live. For a live slot, hopping[j, t] with columns[j, t] = i is the transpose of hopping[i, s] with columns[i, s] = j.
All inputs are finite; a program needn't handle non-finite values.
Results may differ from the reference program's by a relative error of at most 0.0098.
Values may be sent and summed in bfloat16 or wider, within the bound.
No kernel may reach another device: no remote copies, remote signals or barrier semaphores. Data moves between devices by JAX's collectives and lax.ppermute only.
A program may use at most 64 MiB of HBM per device.

```python
import jax
import jax.numpy as jnp
from jax import lax

BLK = 128
REACH = 2
M = 1024
DEG = 12
SLOTS = 4
NBLK = 512
NROWS = 65536


def neighbour_graph(key):
    base_key = jax.random.fold_in(key, 9071)
    density = jax.random.randint(jax.random.fold_in(base_key, 1), (NBLK,), 30, 100)
    edge_rolls = jax.random.randint(jax.random.fold_in(base_key, 2), (NBLK, REACH), 0, 100)
    forward = (edge_rolls < density[:, None]).astype(jnp.int32)
    forward = forward.at[0, :].set(1)
    for reach_step in range(REACH):
        forward = forward.at[NBLK - reach_step - 1, reach_step].set(1)
    backward = jnp.stack([jnp.roll(forward[:, reach_step], reach_step + 1) for reach_step in range(REACH)], axis=1)
    blocks = jnp.arange(NBLK, dtype=jnp.int32)
    offsets = jnp.arange(1, REACH + 1, dtype=jnp.int32)
    targets = jnp.concatenate([jnp.mod(blocks[:, None] + offsets[None, :], NBLK), jnp.mod(blocks[:, None] - offsets[None, :], NBLK)], axis=1)
    live_slot = jnp.concatenate([forward, backward], axis=1)
    order_key = (1 - live_slot) * SLOTS + jnp.arange(SLOTS, dtype=jnp.int32)[None, :]
    slot_order = jnp.argsort(order_key, axis=1, stable=True)
    columns = jnp.take_along_axis(targets, slot_order, axis=1).astype(jnp.int32)
    counts = jnp.sum(live_slot, axis=1).astype(jnp.int32)
    return (columns, counts)


def draw_columns(key, part):
    return neighbour_graph(key)[0]


def draw_counts(key, part):
    return neighbour_graph(key)[1]


def draw_hopping(key, part):
    columns, counts = neighbour_graph(key)
    row_ids = jnp.broadcast_to(jnp.arange(NBLK, dtype=jnp.int32)[:, None], columns.shape)
    low_id = jnp.minimum(row_ids, columns)
    high_id = jnp.maximum(row_ids, columns)
    pair_ids = (low_id * NBLK + high_id).reshape(-1)
    block_key = jax.random.fold_in(key, 5113)

    def one_block(pair_id):
        return jax.random.normal(jax.random.fold_in(block_key, pair_id), (BLK, BLK), jnp.float32)
    drawn = jax.vmap(one_block)(pair_ids).reshape(NBLK, SLOTS, BLK, BLK)
    transposed = (row_ids > columns)[:, :, None, None]
    drawn = jnp.where(transposed, jnp.swapaxes(drawn, 2, 3), drawn)
    hop_scale = 1.0 / jnp.sqrt(jnp.float32(BLK * (SLOTS + 1)))
    return (drawn * hop_scale).astype(jnp.bfloat16)


def level_of(rng, dims, split, smallest, top_value):
    factor_of = 1.0
    for dim, parts in split:
        heights = jax.random.uniform(jax.random.fold_in(jax.random.fold_in(rng, 6), dim), (parts,), jnp.float32, smallest / len(split), top_value / len(split))
        factor_of = factor_of * jnp.repeat(jnp.exp(heights), dims[dim] // parts).reshape((-1,) + (1,) * (len(dims) - 1 - dim))
    return factor_of


def gaussian(stream_key, extent, scale, reach, shards=(), kind=jnp.bfloat16):
    values = jax.random.normal(stream_key, extent, jnp.float32) * scale
    if len(shards) > 0:
        values = level_of(stream_key, extent, shards, -0.22, 0.18) * values
    return jnp.clip(values, min=-reach, max=reach).astype(kind)


def setup_inputs(seed: int = 0) -> dict:
    keys = jax.random.split(jax.random.key(seed), 6)
    return {
        "start_block": gaussian(keys[0], (NROWS, M), 1.0, 6.0, ((0, 128), (1, 2))),
        "onsite": gaussian(keys[1], (NBLK, BLK, BLK), (2 * BLK * (SLOTS + 1)) ** -0.5, 0.15625, ((0, 128),)),
        "hopping": draw_hopping(jax.random.fold_in(keys[5], 71), 0),
        "columns": draw_columns(jax.random.fold_in(keys[5], 71), 0),
        "counts": draw_counts(jax.random.fold_in(keys[5], 71), 0),
    }


filter_low = -0.5
filter_top = 4.0
filter_bottom = -1.6


def filter_coefficients(degree):
    center = 0.5 * (filter_top + filter_low)
    half_width = 0.5 * (filter_top - filter_low)
    sigma_first = half_width / (filter_bottom - center)
    listed = [(sigma_first / half_width, 0.0)]
    sigma_now = sigma_first
    for degree_step in range(1, degree):
        sigma_next = 1.0 / (2.0 / sigma_first - sigma_now)
        listed.append((2.0 * sigma_next / half_width, sigma_now * sigma_next))
        sigma_now = sigma_next
    return center, listed


def apply_operator(vectors, onsite, hopping, columns, counts):
    as_wide = vectors.astype(jnp.float32)
    onsite_wide = onsite.astype(jnp.float32)
    summed = 0.5 * (jnp.einsum("rij,rjc->ric", onsite_wide, as_wide) + jnp.einsum("rji,rjc->ric", onsite_wide, as_wide))
    live_slot = jnp.arange(SLOTS, dtype=jnp.int32)[None, :] < counts[:, None]
    for slot_index in range(SLOTS):
        weights = jnp.where(live_slot[:, slot_index, None, None], hopping[:, slot_index].astype(jnp.float32), jnp.float32(0.0))
        picked = as_wide[columns[:, slot_index].astype(jnp.int32)]
        summed = summed + jnp.einsum("rij,rjc->ric", weights, picked)
    return summed


def reference(start_block, onsite, hopping, columns, counts):
    center, listed = filter_coefficients(DEG)
    current = start_block.reshape(NBLK, BLK, M)
    previous = jnp.zeros((NBLK, BLK, M), jnp.bfloat16)
    for scale_now, carry_back in listed:
        applied = apply_operator(current, onsite, hopping, columns, counts)
        following = scale_now * (applied - center * current.astype(jnp.float32)) - carry_back * previous.astype(jnp.float32)
        following = lax.optimization_barrier(following.astype(jnp.bfloat16))
        previous, current = current, following
    filtered = current.reshape(NROWS, M)
    applied = apply_operator(current, onsite, hopping, columns, counts).astype(jnp.bfloat16).reshape(NROWS, M)
    gram = jnp.dot(filtered.T, filtered, preferred_element_type=jnp.float32) / NROWS
    projected = jnp.dot(filtered.T, applied, preferred_element_type=jnp.float32) / NROWS
    return filtered, gram, projected
```

```python
import functools

import jax
import jax.numpy as jnp
from jax import lax
from jax.experimental import pallas as pl
from jax.experimental.pallas import tpu as pltpu
from jax.sharding import Mesh
from jax.sharding import PartitionSpec as P

DEG = 12
X, Z, Y, V = "atoms_0", "atoms_1", "atoms_2", "vecs"
ATOMS = (X, Z, Y)
REACH = 2
SPAN = 2 * REACH + 1
STREAMS = 2
VLIM = 12 * 1024 * 1024

filter_low = -0.5
filter_top = 4.0
filter_bottom = -1.6


def filter_coefficients(degree):
    center = 0.5 * (filter_top + filter_low)
    half_width = 0.5 * (filter_top - filter_low)
    sigma_first = half_width / (filter_bottom - center)
    listed = [(sigma_first / half_width, 0.0)]
    sigma_now = sigma_first
    for degree_step in range(1, degree):
        sigma_next = 1.0 / (2.0 / sigma_first - sigma_now)
        listed.append((2.0 * sigma_next / half_width, sigma_now * sigma_next))
        sigma_now = sigma_next
    return (center, listed)


CENTER, LISTED = filter_coefficients(DEG)
VMEM = pl.BlockSpec(memory_space=pltpu.VMEM)
SMEM = pl.BlockSpec(memory_space=pltpu.SMEM)


def cost(flops, bytes_accessed):
    return pl.CostEstimate(flops=int(flops), bytes_accessed=int(bytes_accessed), transcendentals=0)


def dot(a, b):
    return lax.dot_general(a, b, (((1,), (0,)), ((), ())), preferred_element_type=jnp.float32)


def dot_t(a, b):
    return lax.dot_general(a, b, (((0,), (0,)), ((), ())), preferred_element_type=jnp.float32)


def band_kernel(total, first_ref, columns_ref, counts_ref, onsite_ref, hopping_ref, band_ref):
    rows, slots = hopping_ref.shape[:2]
    blk = onsite_ref.shape[1]
    for r in range(rows):
        own = onsite_ref[r].astype(jnp.float32)
        diagonal = 0.5 * (own + own.T)
        shift = [
            lax.rem(columns_ref[r, s] - (first_ref[0] + r) + REACH + total, total)
            for s in range(slots)
        ]
        for k in range(SPAN):
            block = diagonal if k == REACH else jnp.zeros((blk, blk), jnp.float32)
            for s in range(slots):
                hit = jnp.logical_and(shift[s] == k, s < counts_ref[r])
                weight = jnp.where(hit, jnp.float32(1.0), jnp.float32(0.0))
                block = block + weight * hopping_ref[r, s].astype(jnp.float32)
            band_ref[r, :, k * blk : (k + 1) * blk] = block.astype(jnp.bfloat16)


def make_band(onsite, hopping, columns, counts, first, total):
    rows, blk = onsite.shape[:2]
    return pl.pallas_call(
        functools.partial(band_kernel, total),
        out_shape=jax.ShapeDtypeStruct((rows, blk, SPAN * blk), jnp.bfloat16),
        in_specs=[SMEM, SMEM, SMEM, VMEM, VMEM],
        out_specs=VMEM,
        compiler_params=pltpu.CompilerParams(vmem_limit_bytes=VLIM),
        cost_estimate=cost(8e8, 2e6),
        name="band",
    )(first, columns, counts, onsite, hopping)


def at(index, size, count=1):
    return slice(index * size, (index + count) * size)


def first_kernel(coef, rows, blk, left, own, right, band, now_out, window):
    side = rows * blk
    rim = REACH * blk
    window[0:rim] = left[...]
    window[rim : rim + side] = own[...]
    window[rim + side : 2 * rim + side] = right[...]

    def body(r):
        applied = dot(band[r], window[at(r, blk, SPAN), :])
        here = own[at(r, blk), :].astype(jnp.float32)
        now_out[at(r, blk), :] = (coef * (applied - CENTER * here)).astype(jnp.bfloat16)

    for r in range(rows):
        body(r)


def first_step(left, own, right, band):
    rows, blk = band.shape[:2]
    width = own.shape[1]
    return pl.pallas_call(
        functools.partial(first_kernel, LISTED[0][0], rows, blk),
        out_shape=(
            jax.ShapeDtypeStruct((rows * blk, width), jnp.bfloat16),
            jax.ShapeDtypeStruct(((rows + 2 * REACH) * blk, width), jnp.bfloat16),
        ),
        in_specs=[VMEM] * 4,
        out_specs=(VMEM, VMEM),
        compiler_params=pltpu.CompilerParams(vmem_limit_bytes=VLIM),
        cost_estimate=cost(2 * rows * blk * SPAN * blk * width, 2e6),
        name="first",
    )(left, own, right, band)


def pair_kernel(coefs, rows, blk, left, own, right, prev, band, now_out, mid_out, window, *ext):
    (scale_a, carry_a), second = coefs
    mid = ext[0] if ext else mid_out
    side = rows * blk
    window[0:side] = left[...]
    window[side : 2 * side] = own[...]
    window[2 * side : 3 * side] = right[...]

    def inner(e):
        base = e + (rows - 2 * REACH)
        applied = dot(band[e], window[at(base, blk, SPAN), :])
        here = window[at(base + REACH, blk), :].astype(jnp.float32)
        value = scale_a * (applied - CENTER * here)
        value = value - carry_a * prev[at(e, blk), :].astype(jnp.float32)
        mid[at(e, blk), :] = value.astype(jnp.bfloat16)

    for e in range(rows + 2 * REACH):
        inner(e)

    def outer(r):
        value = dot(band[r + REACH], mid[at(r, blk, SPAN), :])
        if second is not None:
            here = mid[at(r + REACH, blk), :].astype(jnp.float32)
            value = second[0] * (value - CENTER * here)
            value = value - second[1] * own[at(r, blk), :].astype(jnp.float32)
        now_out[at(r, blk), :] = value.astype(jnp.bfloat16)

    for r in range(rows):
        outer(r)
    if ext:
        mid_out[...] = mid[REACH * blk : (REACH + rows) * blk]


def pair_step(coefs, left, own, right, prev, band):
    ext, blk = band.shape[:2]
    rows = ext - 2 * REACH
    width = own.shape[1]
    last = coefs[1] is None
    scratch = [pltpu.VMEM((3 * rows * blk, width), jnp.bfloat16)]
    if last:
        scratch.append(pltpu.VMEM((ext * blk, width), jnp.bfloat16))
    return pl.pallas_call(
        functools.partial(pair_kernel, coefs, rows, blk),
        out_shape=(
            jax.ShapeDtypeStruct((rows * blk, width), jnp.bfloat16),
            jax.ShapeDtypeStruct(((rows if last else ext) * blk, width), jnp.bfloat16),
        ),
        in_specs=[VMEM] * 5,
        out_specs=(VMEM, VMEM),
        scratch_shapes=scratch,
        compiler_params=pltpu.CompilerParams(vmem_limit_bytes=VLIM),
        cost_estimate=cost(2 * (ext + rows) * blk * SPAN * blk * width, 3e6),
        name="pair",
    )(left, own, right, prev, band)


def product_kernel(split, me_ref, own, other, rhs, *refs):
    outs, full, result = refs[:4], refs[4], refs[5]
    width = own.shape[1]
    full[:, pl.ds(pl.multiple_of(me_ref[0] * width, width), width)] = own[...]
    full[:, pl.ds(pl.multiple_of((1 - me_ref[0]) * width, width), width)] = other[...]
    for d, out in enumerate(outs):
        part = lax.rem(me_ref[1] + d, 4)
        size = 2 * width // 4
        if split == 0:
            columns = pl.ds(pl.multiple_of(part * size, size), size)
            out[...] = dot_t(full[:, columns], rhs[...]).astype(jnp.bfloat16)
        else:
            if d == 0:
                for q in range(4):
                    piece = dot_t(full[:, q * size : (q + 1) * size], rhs[...])
                    result[q * size // 32 : (q + 1) * size // 32] = piece.reshape(
                        size // 32, 4, 8, rhs.shape[1]
                    )
            out[...] = result[:, part].reshape(size, rhs.shape[1]).astype(jnp.bfloat16)


def product(split, me, own, other, rhs):
    depth, width = own.shape
    scratch = [pltpu.VMEM((depth, 2 * width), jnp.bfloat16)]
    scratch.append(pltpu.VMEM((2 * width // 32, 4, 8, rhs.shape[1]) if split else (8, 128), jnp.float32))
    return pl.pallas_call(
        functools.partial(product_kernel, split),
        out_shape=[jax.ShapeDtypeStruct((width // 2, rhs.shape[1]), jnp.bfloat16)] * 4,
        in_specs=[SMEM, VMEM, VMEM, VMEM],
        out_specs=[VMEM] * 4,
        scratch_shapes=scratch,
        compiler_params=pltpu.CompilerParams(vmem_limit_bytes=VLIM),
        cost_estimate=cost(4 * depth * width * rhs.shape[1], 3e6),
        name="product",
    )(me, own, other, rhs)


def shifted(x, by):
    count = lax.axis_size(ATOMS)
    return lax.ppermute(x, ATOMS, [(i, (i + by) % count) for i in range(count)])


def exchanged_sum(parts, axis):
    count = lax.axis_size(axis)
    got = [
        lax.ppermute(parts[d], axis, [(i, (i + d) % count) for i in range(count)])
        for d in (1, 3, 2)
    ]
    total = parts[0].astype(jnp.float32)
    for piece in got:
        total = total + piece.astype(jnp.float32)
    return total.astype(jnp.bfloat16)


def parts_of(x, axis, dim):
    count = lax.axis_size(axis)
    me = lax.axis_index(axis)
    return [
        lax.dynamic_index_in_dim(x, lax.rem(me + d, count), dim, keepdims=False)
        for d in range(count)
    ]


def shards(start_block, onsite, hopping, columns, counts):
    rows, blk = onsite.shape[:2]
    height, width = start_block.shape
    total_blocks = rows * lax.axis_size(ATOMS)
    first = (lax.axis_index(ATOMS) * rows).astype(jnp.int32).reshape(1)

    v = lax.axis_index(V)
    part = width // STREAMS
    rim = REACH * blk
    streams = [start_block[:, i * part : (i + 1) * part] for i in range(STREAMS)]
    halos = [(shifted(y[height - rim :], 1), shifted(y[:rim], -1)) for y in streams]
    band = make_band(onsite, hopping, columns, counts, first, total_blocks)
    states = [first_step(l, y, r, band) for y, (l, r) in zip(streams, halos)]
    band = jnp.concatenate(
        [shifted(band[rows - REACH :], 1), band, shifted(band[:REACH], -1)], axis=0
    )
    for k in range(1, DEG, 2):
        coefs = (LISTED[k], LISTED[k + 1] if k + 1 < DEG else None)
        halos = [(shifted(now, 1), shifted(now, -1)) for now, mid in states]
        states = [
            pair_step(coefs, l, now, r, mid, band) for (now, mid), (l, r) in zip(states, halos)
        ]
    swap = [(0, 1), (1, 0)]
    other = jnp.concatenate([lax.ppermute(f, V, swap) for applied, f in states], axis=1)
    filtered = jnp.concatenate([f for applied, f in states], axis=1)
    applied = jnp.concatenate([applied for applied, f in states], axis=1)
    at_x = jnp.stack([v, lax.axis_index(X)]).astype(jnp.int32)
    at_y = jnp.stack([v, lax.axis_index(Y)]).astype(jnp.int32)
    gram = exchanged_sum(product(0, at_x, filtered, other, filtered), X)
    proj = exchanged_sum(product(1, at_y, filtered, other, applied), Y)

    nx, nz, ny = lax.axis_size(X), lax.axis_size(Z), lax.axis_size(Y)
    leaf = 2 * width // (nx * nz * ny)
    gram = exchanged_sum(parts_of(gram.reshape(nz, ny, leaf, width), Y, 1), Y)
    proj = exchanged_sum(parts_of(proj.reshape(nx, nz, leaf, width), X, 0), X)
    both = jnp.stack([gram, proj], axis=1)
    both = lax.all_to_all(both, Z, 0, 0, tiled=False)
    both = jnp.sum(both.astype(jnp.float32), axis=0)
    scale = 1.0 / (total_blocks * blk)
    return (filtered, both[0] * scale, both[1] * scale)


def solution(mesh):
    split = Mesh(mesh.devices.reshape(4, 8, 4, mesh.shape["vecs"]), (X, Z, Y, V))
    placed = (
        P(ATOMS, V),
        P(ATOMS, None, None),
        P(ATOMS, None, None, None),
        P(ATOMS, None),
        P(ATOMS),
    )
    return jax.shard_map(
        shards,
        mesh=split,
        in_specs=placed,
        out_specs=(P(ATOMS, V), P(ATOMS, V), P(ATOMS, V)),
        check_vma=False,
    )
```

```python
import functools

import jax
import jax.numpy as jnp
from jax import lax
from jax.experimental import pallas as pl
from jax.experimental.pallas import tpu as pltpu
from jax.sharding import Mesh
from jax.sharding import PartitionSpec as P


DEG = 12
X, Z, Y, V = "atoms_0", "atoms_1", "atoms_2", "vecs"
ATOMS = (X, Z, Y)
REACH = 2
SPAN = 2 * REACH + 1
STREAMS = (256, 256)


VLIM = 4 * 1024 * 1024

filter_low = -0.5
filter_top = 4.0
filter_bottom = -1.6


def filter_coefficients(degree):
    center = 0.5 * (filter_top + filter_low)
    half_width = 0.5 * (filter_top - filter_low)
    sigma_first = half_width / (filter_bottom - center)
    listed = [(sigma_first / half_width, 0.0)]
    sigma_now = sigma_first
    for _ in range(1, degree):
        sigma_next = 1.0 / (2.0 / sigma_first - sigma_now)
        listed.append((2.0 * sigma_next / half_width, sigma_now * sigma_next))
        sigma_now = sigma_next
    return (center, listed)


CENTER, LISTED = filter_coefficients(DEG)
VMEM = pl.BlockSpec(memory_space=pltpu.VMEM)
SMEM = pl.BlockSpec(memory_space=pltpu.SMEM)


def cost(flops, bytes_accessed):
    return pl.CostEstimate(flops=int(flops), bytes_accessed=int(bytes_accessed), transcendentals=0)


def dot(a, b):
    return lax.dot_general(a, b, (((1,), (0,)), ((), ())), preferred_element_type=jnp.float32)


def dot_t(a, b):
    return lax.dot_general(a, b, (((0,), (0,)), ((), ())), preferred_element_type=jnp.float32)


def band_kernel(total, first_ref, columns_in, counts_in, onsite_in, hopping_in, band_ref, *scratch):
    arrays, sems = scratch[:4], scratch[4:]
    pairs = zip((columns_in, counts_in, onsite_in, hopping_in), arrays, sems)
    copies = [pltpu.make_async_copy(source, target, sem) for source, target, sem in pairs]
    for copy in copies:
        copy.start()
    for copy in copies:
        copy.wait()
    columns_ref, counts_ref, onsite_ref, hopping_ref = arrays
    rows, slots = hopping_ref.shape[:2]
    blk = onsite_ref.shape[1]

    def one_row(r, carry):
        own = onsite_ref[r].astype(jnp.float32)
        diagonal = 0.5 * (own + own.T)
        shift = [
            lax.rem(columns_ref[r, s] - (first_ref[0] + r) + REACH + total, total)
            for s in range(slots)
        ]
        for k in range(SPAN):
            block = diagonal if k == REACH else jnp.zeros((blk, blk), jnp.float32)
            for s in range(slots):
                hit = jnp.logical_and(shift[s] == k, s < counts_ref[r])
                weight = jnp.where(hit, jnp.float32(1.0), jnp.float32(0.0))
                block = block + weight * hopping_ref[r, s].astype(jnp.float32)
            band_ref[r, :, k * blk : (k + 1) * blk] = block.astype(jnp.bfloat16)
        return carry

    lax.fori_loop(0, rows, one_row, 0)


def make_band(onsite, hopping, columns, counts, first, total):
    rows, blk = onsite.shape[:2]
    return pl.pallas_call(
        functools.partial(band_kernel, total),
        out_shape=jax.ShapeDtypeStruct((rows, blk, SPAN * blk), jnp.bfloat16),
        in_specs=[SMEM] + [pl.BlockSpec(memory_space=pltpu.HBM)] * 4,
        out_specs=VMEM,
        scratch_shapes=[
            pltpu.SMEM(columns.shape, columns.dtype),
            pltpu.SMEM(counts.shape, counts.dtype),
            pltpu.VMEM(onsite.shape, onsite.dtype),
            pltpu.VMEM(hopping.shape, hopping.dtype),
        ]
        + [pltpu.SemaphoreType.DMA] * 4,
        compiler_params=pltpu.CompilerParams(vmem_limit_bytes=60 * 1024 * 1024),
        cost_estimate=cost(8e8, 2e6),
        name="band",
    )(first, columns, counts, onsite, hopping)


def at(index, size, count=1):
    return pl.ds(pl.multiple_of(index * size, size), count * size)


def fill(window, odd_ref, near, own, far):
    side, mine = near.shape[0], own.shape[0]
    span = side + mine
    window[pl.ds(pl.multiple_of((1 - odd_ref[0]) * span, 128), side)] = near[...]
    window[pl.ds(pl.multiple_of(odd_ref[0] * span, 128), side)] = far[...]
    window[side : side + mine] = own[...]


def first_kernel(coef, rows, blk, odd_ref, near, own, far, band, *refs):
    outs, window = refs[:-1], refs[-1]
    count = len(outs) // 2
    fill(window, odd_ref, near, own, far)
    start = 0
    for now_out, mid_out in zip(outs[:count], outs[count:]):
        columns = slice(start, start + now_out.shape[1])
        start = columns.stop
        mid_out[...] = window[:, columns]
        for r in range(rows):
            applied = dot(band[r], mid_out[at(r, blk, SPAN), :])
            here = mid_out[at(r + REACH, blk), :].astype(jnp.float32)
            now_out[at(r, blk), :] = (coef * (applied - CENTER * here)).astype(jnp.bfloat16)


def first_step(odd, near, own, far, band):
    rows, blk = band.shape[:2]
    height, width = own.shape
    outs = pl.pallas_call(
        functools.partial(first_kernel, LISTED[0][0], rows, blk),
        out_shape=[jax.ShapeDtypeStruct((height, w), jnp.bfloat16) for w in STREAMS]
        + [jax.ShapeDtypeStruct((height + 2 * REACH * blk, w), jnp.bfloat16) for w in STREAMS],
        in_specs=[SMEM] + [VMEM] * 4,
        out_specs=[VMEM] * (2 * len(STREAMS)),
        scratch_shapes=[pltpu.VMEM((height + 2 * REACH * blk, width), jnp.bfloat16)],
        compiler_params=pltpu.CompilerParams(vmem_limit_bytes=VLIM),
        cost_estimate=cost(2 * rows * blk * SPAN * blk * width, 2e6),
        name="first",
    )(odd, near, own, far, band)
    return list(zip(outs[: len(STREAMS)], outs[len(STREAMS) :]))


def pair_kernel(coefs, rows, blk, odd_ref, near, own, far, prev, band, now_out, mid_out, window, *ext):
    (scale_a, carry_a), second = coefs
    mid = ext[0] if ext else mid_out
    fill(window, odd_ref, near, own, far)

    def inner(e):
        base = e + (rows - 2 * REACH)
        applied = dot(band[e], window[at(base, blk, SPAN), :])
        here = window[at(base + REACH, blk), :].astype(jnp.float32)
        value = scale_a * (applied - CENTER * here)
        value = value - carry_a * prev[at(e, blk), :].astype(jnp.float32)
        mid[at(e, blk), :] = value.astype(jnp.bfloat16)

    def several(i, carry):
        for u in range(rows):
            inner(i * rows + u)
        return carry

    lax.fori_loop(0, (rows + 2 * REACH) // rows, several, 0)

    def outer(r):
        value = dot(band[r + REACH], mid[at(r, blk, SPAN), :])
        if second is not None:
            here = mid[at(r + REACH, blk), :].astype(jnp.float32)
            value = second[0] * (value - CENTER * here)
            value = value - second[1] * own[at(r, blk), :].astype(jnp.float32)
        now_out[at(r, blk), :] = value.astype(jnp.bfloat16)

    for r in range(rows):
        outer(r)
    if ext:
        mid_out[...] = mid[REACH * blk : (REACH + rows) * blk]


def pair_step(coefs, odd, near, own, far, prev, band):
    ext, blk = band.shape[:2]
    rows = ext - 2 * REACH
    width = own.shape[1]
    last = coefs[1] is None
    scratch = [pltpu.VMEM((3 * rows * blk, width), jnp.bfloat16)]
    if last:
        scratch.append(pltpu.VMEM((ext * blk, width), jnp.bfloat16))
    return pl.pallas_call(
        functools.partial(pair_kernel, coefs, rows, blk),
        out_shape=(
            jax.ShapeDtypeStruct((rows * blk, width), jnp.bfloat16),
            jax.ShapeDtypeStruct(((rows if last else ext) * blk, width), jnp.bfloat16),
        ),
        in_specs=[SMEM] + [VMEM] * 5,
        out_specs=(VMEM, VMEM),
        scratch_shapes=scratch,
        compiler_params=pltpu.CompilerParams(vmem_limit_bytes=VLIM),
        cost_estimate=cost(2 * (ext + rows) * blk * SPAN * blk * width, 3e6),
        name="pair",
    )(odd, near, own, far, prev, band)


def product_kernel(count, me_ref, *refs):
    own, other, applied = refs[:count], refs[count : 2 * count], refs[2 * count : 3 * count]
    gram_outs, proj_outs = refs[3 * count : 3 * count + 4], refs[3 * count + 4 : 3 * count + 8]
    full, result = refs[3 * count + 8 :]
    width = result.shape[3]
    size = 2 * width // 4
    for pieces, start in ((own, me_ref[0] * width), (other, (1 - me_ref[0]) * width)):
        for piece in pieces:
            full[:, pl.ds(pl.multiple_of(start, 128), piece.shape[1])] = piece[...]
            start = start + piece.shape[1]
    for d, out in enumerate(gram_outs):
        columns = at(lax.bitwise_xor(me_ref[1], d), size)
        start = 0
        for piece in own:
            stop = start + piece.shape[1]
            out[:, start:stop] = dot_t(full[:, columns], piece[...]).astype(jnp.bfloat16)
            start = stop
    for q in range(4):
        start = 0
        for piece in applied:
            stop = start + piece.shape[1]
            value = dot_t(full[:, q * size : (q + 1) * size], piece[...])
            result[:, :, :, start:stop] = value.reshape(size // 32, 4, 8, stop - start)
            start = stop
        for d, out in enumerate(proj_outs):
            mine = result[:, lax.bitwise_xor(me_ref[2], d)].reshape(size // 4, width)
            out[q * size // 4 : (q + 1) * size // 4] = mine.astype(jnp.bfloat16)


def products(me, own, other, applied):
    depth = own[0].shape[0]
    width = sum(STREAMS)
    part = jax.ShapeDtypeStruct((width // 2, width), jnp.bfloat16)
    outs = pl.pallas_call(
        functools.partial(product_kernel, len(STREAMS)),
        out_shape=[part] * 8,
        in_specs=[SMEM] + [VMEM] * (3 * len(STREAMS)),
        out_specs=[VMEM] * 8,
        scratch_shapes=[
            pltpu.VMEM((depth, 2 * width), jnp.bfloat16),
            pltpu.VMEM((width // 64, 4, 8, width), jnp.float32),
        ],
        compiler_params=pltpu.CompilerParams(vmem_limit_bytes=VLIM),
        cost_estimate=cost(8 * depth * width * width, 3e6),
        name="products",
    )(me, *own, *other, *applied)
    return outs[:4], outs[4:]


def traded(to_right, to_left, odd):
    count = lax.axis_size(ATOMS)
    near = [(i, i ^ 1) for i in range(count)]
    far = [(i, ((i + 1) ^ 1) - 1) for i in range(count)]
    far = [(i, j % count) for i, j in far]
    if to_right is to_left:
        first = second = to_right
    else:
        first = jnp.where(odd, to_left, to_right)
        second = jnp.where(odd, to_right, to_left)
    from_near = lax.ppermute(first, ATOMS, near)
    from_far = lax.ppermute(second, ATOMS, far)
    return from_near, from_far


def with_other_half(piece, v):
    other = lax.ppermute(piece, V, [(0, 1), (1, 0)])
    return jnp.where(
        v == 0, jnp.concatenate([piece, other], axis=1), jnp.concatenate([other, piece], axis=1)
    )


def summed(pieces):
    total = pieces[0].astype(jnp.float32)
    for piece in pieces[1:]:
        total = total + piece.astype(jnp.float32)
    return total.astype(jnp.bfloat16)


def parts_of(x, axis, dim):
    me = lax.axis_index(axis)
    return [
        lax.dynamic_index_in_dim(x, jnp.bitwise_xor(me, d), dim, keepdims=False)
        for d in range(lax.axis_size(axis))
    ]


def exchanged(parts, axis):
    count = lax.axis_size(axis)
    order = sorted(range(1, count), key=lambda d: (d != 2, d))
    return [parts[0]] + [
        lax.ppermute(parts[d], axis, [(i, i ^ d) for i in range(count)]) for d in order
    ]


def shards(start_block, onsite, hopping, columns, counts):
    rows, blk = onsite.shape[:2]
    height, width = start_block.shape
    total_blocks = rows * lax.axis_size(ATOMS)
    first = (lax.axis_index(ATOMS) * rows).astype(jnp.int32).reshape(1)

    rim = REACH * blk
    is_odd = lax.rem(lax.axis_index(ATOMS), 2)
    odd = is_odd.astype(jnp.int32).reshape(1)
    is_odd = is_odd == 1
    near, far = traded(start_block[height - rim :], start_block[:rim], is_odd)
    band = make_band(onsite, hopping, columns, counts, first, total_blocks)
    own = start_block + lax.div(lax.axis_index(V), 2).astype(jnp.bfloat16)
    states = first_step(odd, near, own, far, band)
    v = lax.axis_index(V)
    half = lax.dynamic_slice_in_dim(band, v * (blk // 2), blk // 2, axis=1)
    halves = traded(half[rows - REACH :], half[:REACH], is_odd)
    both = with_other_half(jnp.concatenate(halves, axis=0), v)
    near, far = both[:REACH], both[REACH:]
    band = jnp.concatenate(
        [jnp.where(is_odd, near, far), band, jnp.where(is_odd, far, near)], axis=0
    )
    for k in range(1, DEG, 2):
        coefs = (LISTED[k], LISTED[k + 1] if k + 1 < DEG else None)
        halos = [traded(now, now, is_odd) for now, mid in states]
        old, states = states, []
        for (now, mid), (n, f) in zip(old, halos):
            states.append(pair_step(coefs, odd, n, now, f, mid, band))
    own = [f for applied, f in states]
    other = [lax.ppermute(f, V, [(0, 1), (1, 0)]) for f in own]
    me = jnp.stack([lax.axis_index(a) for a in (V, X, Y)]).astype(jnp.int32)
    nx, nz, ny = lax.axis_size(X), lax.axis_size(Z), lax.axis_size(Y)
    leaf = 2 * width // (nx * nz * ny)
    gram, proj = products(me, own, other, [applied for applied, f in states])
    gram = summed(exchanged(gram, X)).reshape(nz, ny, leaf, width)
    proj = summed(exchanged(proj, Y)).reshape(nx, nz, leaf, width)
    gram = summed(exchanged(parts_of(gram, Y, 1), Y))
    proj = summed(exchanged(parts_of(proj, X, 0), X))
    both = jnp.stack([gram, proj], axis=1)
    both = jnp.sum(lax.all_to_all(both, Z, 0, 0).astype(jnp.float32), axis=0)
    scale = 1.0 / (total_blocks * blk)
    filtered = jnp.concatenate(own, axis=1)
    return (filtered, both[0] * scale, both[1] * scale)


def solution(mesh):
    split = Mesh(mesh.devices.reshape(4, 8, 4, mesh.shape["vecs"]), (X, Z, Y, V))
    placed = (
        P(ATOMS, V),
        P(ATOMS, None, None),
        P(ATOMS, None, None, None),
        P(ATOMS, None),
        P(ATOMS),
    )

    return jax.shard_map(
        shards,
        mesh=split,
        in_specs=placed,
        out_specs=(P(ATOMS, V), P(ATOMS, V), P(ATOMS, V)),
        check_vma=False,
    )
```
